512 devices in a mesh: cp: 128 (over z, x, core), dp: 4 (over y).
Axes of the slice: x: 4, y: 4, z: 16, core: 2. Of those that a mesh axis runs over, the one named last changes fastest.
Arguments:
- queries: bfloat16 [196608, 1024], P('cp', 'dp'), may hold values from -112 to 112, as said below
- keys: bfloat16 [196608, 128], P('cp'), may hold values from -7 to 7
- values: bfloat16 [196608, 128], P('cp'), may hold values from -6 to 6
- out_grad: bfloat16 [196608, 1024], P('cp', 'dp'), may hold values from -6 to 6
- lengths: int32 [384, 4], P('cp'), may hold values from 1 to 509, as said below
- hop_table: int32 [128, 3], P('cp'), may hold values from 0 to 2, each once within a row
Outputs:
- attn_out: bfloat16 [196608, 1024], P('cp', 'dp')
- query_grad: bfloat16 [196608, 1024], P('cp', 'dp')
- key_grad: bfloat16 [196608, 128], P('cp')
- value_grad: bfloat16 [196608, 128], P('cp')
- row_stats: float32 [8, 196608], P('dp', 'cp')
The draws below stay inside these ranges and needn't reach their ends.
Inputs may be any that keep to these rules, and one draw needn't show every extreme that they name: Built so that queries and keys stay within this range. `lengths`: each row sums to 512; every slot of the first quarter of the cp loaders begins with a document of at least 384 rows. `hop_table`: each row names every hop once.
All inputs are finite; a program needn't handle non-finite values.
Results may differ from the reference program's by a relative error of at most 0.006.
Values may be sent and summed in bfloat16 or wider, within the bound.
No kernel may reach another device: no remote copies, remote signals or barrier semaphores. Data moves between devices by JAX's collectives and lax.ppermute only.
A program may use at most 128 MiB of HBM per device.

```python
import jax
import jax.numpy as jnp
from jax import lax

HEADS = 8
HD = 128
SLOT = 512
DOCS = 4
HOPS = 3
TOKENS = 196608
N_CP = 128


def query_key_pair(key):
    base_key = jax.random.fold_in(key, 1234)
    key_draw, query_draw = jax.random.split(base_key, 2)
    key_rows = jnp.clip(jax.random.normal(key_draw, (TOKENS, HD), jnp.float32), -6.0, 6.0)
    query_rows = jnp.clip(jax.random.normal(query_draw, (TOKENS, HEADS, HD), jnp.float32), -6.0, 6.0)
    return (query_rows.reshape(TOKENS, HEADS * HD), key_rows)


def draw_queries(key, part):
    return query_key_pair(key)[0].astype(jnp.bfloat16)


def draw_keys(key, part):
    return query_key_pair(key)[1].astype(jnp.bfloat16)


def split_slot(slot_key, long_slot):
    wide_key, narrow_key = jax.random.split(slot_key)
    spread_cuts = jax.random.permutation(wide_key, SLOT - 1)[:DOCS - 1] + 1
    narrow_cuts = jax.random.permutation(narrow_key, SLOT // 4 - 1)[:DOCS - 1] + (SLOT - SLOT // 4 + 1)
    cut_points = jnp.sort(jnp.where(long_slot, narrow_cuts, spread_cuts).astype(jnp.int32))
    boundary = jnp.concatenate([jnp.zeros((1,), jnp.int32), cut_points, jnp.full((1,), SLOT, jnp.int32)])
    return boundary[1:] - boundary[:-1]


def draw_lengths(key, part):
    slot_count = TOKENS // SLOT
    loader_count = slot_count // HOPS
    base_key = jax.random.fold_in(key, 77)
    slot_keys = jax.random.split(base_key, slot_count)
    loader_of = jnp.arange(slot_count, dtype=jnp.int32) // HOPS
    long_slot = loader_of < loader_count // 4
    return jax.vmap(split_slot)(slot_keys, long_slot).astype(jnp.int32)


def block_levels(key, dims, cuts, least, high):
    loudness, own = 1.0, jax.random.fold_in(key, 6)
    for dim, parts in cuts:
        steps = jnp.exp(jax.random.uniform(jax.random.fold_in(own, dim), (parts,), jnp.float32, least / len(cuts), high / len(cuts)))
        loudness = loudness * jnp.repeat(steps, dims[dim] // parts).reshape([-1 if axis == dim else 1 for axis in range(len(dims))])
    return loudness


def scatter_about(rng, dims, deviation, limit, cuts=(), held_as=jnp.bfloat16):
    drawn = deviation * jax.random.normal(rng, dims, jnp.float32)
    if cuts:
        drawn = drawn * block_levels(rng, dims, cuts, -0.22, 0.18)
    return jnp.clip(drawn, -limit, limit).astype(held_as)


def setup_inputs(seed: int = 0) -> dict:
    splits = jax.random.split(jax.random.key(seed), 7)
    queries = draw_queries(jax.random.fold_in(splits[6], 71), 0)
    keys = draw_keys(jax.random.fold_in(splits[6], 71), 0)
    values = scatter_about(splits[2], (TOKENS, HD), 1.0, 6.0, ((0, 128),))
    out_grad = scatter_about(splits[3], (TOKENS, HEADS * HD), 1.0, 6.0, ((0, 128), (1, 4)))
    lengths = draw_lengths(jax.random.fold_in(splits[6], 71), 0)
    hop_table = jax.vmap(lambda own: jax.random.permutation(own, HOPS))(jax.random.split(splits[5], N_CP)).reshape((N_CP, HOPS)).astype(jnp.int32)
    return dict(queries=queries, keys=keys, values=values, out_grad=out_grad, lengths=lengths, hop_table=hop_table)


def segment_rows(doc_lengths, slot_rows):
    doc_ends = jnp.cumsum(doc_lengths)
    position = jnp.arange(slot_rows, dtype=jnp.int32)
    return jnp.sum((position[:, None] >= doc_ends[None, :]).astype(jnp.int32), axis=1)


def slot_pass(queries, keys, values, out_grad, doc_lengths):
    slot_rows = queries.shape[0]
    head_count = queries.shape[1] // HD
    score_scale = HD ** -0.5
    segment = segment_rows(doc_lengths, slot_rows)
    query_heads = queries.astype(jnp.float32).reshape(slot_rows, head_count, HD)
    grad_heads = out_grad.astype(jnp.float32).reshape(slot_rows, head_count, HD)
    key_rows = keys.astype(jnp.float32)
    value_rows = values.astype(jnp.float32)
    position = jnp.arange(slot_rows, dtype=jnp.int32)
    allowed = (segment[:, None] == segment[None, :]) & (position[:, None] >= position[None, :])
    scores = jnp.einsum("shd,td->hst", query_heads, key_rows) * score_scale
    scores = jnp.where(allowed[None], scores, -jnp.inf)
    row_max = jnp.max(scores, axis=2, keepdims=True)
    exp_scores = jnp.exp(scores - row_max)
    row_total = jnp.sum(exp_scores, axis=2, keepdims=True)
    softmax = exp_scores / row_total
    log_total = (row_max + jnp.log(row_total))[:, :, 0]
    weights = softmax.astype(jnp.bfloat16).astype(jnp.float32)
    output = jnp.einsum("hst,td->shd", weights, value_rows)
    row_delta = jnp.sum(grad_heads * output, axis=2)
    prob_grad = jnp.einsum("shd,td->hst", grad_heads, value_rows)
    score_grad = (softmax * (prob_grad - jnp.transpose(row_delta)[:, :, None])).astype(jnp.bfloat16).astype(jnp.float32)
    query_grad = jnp.einsum("hst,td->shd", score_grad, key_rows) * score_scale
    key_grad = jnp.einsum("hst,shd->td", score_grad, query_heads) * score_scale
    value_grad = jnp.einsum("hst,shd->td", weights, grad_heads)
    flat_shape = (slot_rows, head_count * HD)
    return (output.reshape(flat_shape).astype(jnp.bfloat16), query_grad.reshape(flat_shape).astype(jnp.bfloat16),
            key_grad.astype(jnp.bfloat16), value_grad.astype(jnp.bfloat16), log_total)


def run_slot(packed):
    return slot_pass(packed[0], packed[1], packed[2], packed[3], packed[4])


def reference(queries, keys, values, out_grad, lengths, hop_table):
    slot_count = TOKENS // SLOT
    width = HEADS * HD
    results = lax.map(run_slot, (queries.reshape(slot_count, SLOT, width), keys.reshape(slot_count, SLOT, HD),
                                 values.reshape(slot_count, SLOT, HD), out_grad.reshape(slot_count, SLOT, width), lengths))
    attn_out = results[0].reshape(TOKENS, width)
    query_grad = results[1].reshape(TOKENS, width)
    key_grad = results[2].reshape(TOKENS, HD)
    value_grad = results[3].reshape(TOKENS, HD)
    stats = results[4].reshape(N_CP, HOPS, HEADS, SLOT)
    loader_ids = jnp.arange(N_CP, dtype=jnp.int32)
    slot_ids = jnp.arange(HOPS, dtype=jnp.int32)
    gathered = []
    for hop_number in range(HOPS):
        distance = 0 if hop_number == 0 else N_CP >> (HOPS - hop_number)
        source = ((loader_ids - distance) % N_CP).astype(jnp.int32)
        chosen = jnp.sum(jnp.where(hop_table[source] == hop_number, slot_ids[None, :], 0), axis=1).astype(jnp.int32)
        gathered.append(stats[source, chosen])
    owner_stats = jnp.stack(gathered, axis=1)
    row_stats = jnp.transpose(owner_stats, (2, 0, 1, 3)).reshape(HEADS, TOKENS)
    return attn_out, query_grad, key_grad, value_grad, row_stats
```

```python
import functools
import math

import jax
import jax.numpy as jnp
from jax import lax
from jax.experimental import pallas as pl
from jax.experimental.pallas import tpu as pltpu
from jax.sharding import PartitionSpec as P

BLOCK = 128


def slot_body(
    order,
    lengths,
    queries,
    keys,
    values,
    out_grad,
    attn_out,
    query_grad,
    partial,
    stats,
    key_sum,
    value_sum,
    *,
    heads,
    scale,
):
    rows, head_size = keys.shape
    blocks = rows // BLOCK
    wide = heads * BLOCK
    slot = order[pl.program_id(0)]
    first_end = lengths[slot, 0]
    second_end = first_end + lengths[slot, 1]
    third_end = second_end + lengths[slot, 2]
    value_cols = jnp.transpose(values[...])
    key_cols = jnp.transpose(keys[...])
    to_exp2 = scale * math.log2(math.e)
    nt = (((1,), (1,)), ((), ()))
    nn = (((1,), (0,)), ((), ()))
    lane = lax.broadcasted_iota(jnp.int32, (1, wide), 1) % BLOCK

    def stacked(ref, begin):
        return jnp.concatenate(
            [
                ref[begin : begin + BLOCK, h * head_size : (h + 1) * head_size]
                for h in range(heads)
            ],
            axis=0,
        )

    for block in reversed(range(blocks)):
        begin = block * BLOCK
        span = begin + BLOCK
        query_rows = stacked(queries, begin)
        grad_rows = stacked(out_grad, begin)
        row = lane + begin
        start = jnp.where(
            row >= third_end,
            third_end,
            jnp.where(row >= second_end, second_end, jnp.where(row >= first_end, first_end, 0)),
        )
        col = lax.broadcasted_iota(jnp.int32, (span, wide), 0)
        allowed = (col >= start) & (col <= row)
        scores = lax.dot_general(
            keys[0:span, :], query_rows, nt, preferred_element_type=jnp.float32
        )
        scores = jnp.where(allowed, scores, -jnp.inf)
        row_max = jnp.max(scores, axis=0, keepdims=True)
        exp_scores = jnp.exp2((scores - row_max) * to_exp2)
        row_total = jnp.sum(exp_scores, axis=0, keepdims=True)
        softmax = exp_scores * (1.0 / row_total)
        log_total = row_max * scale + jnp.log(row_total)
        for h in range(heads):
            stats[0, h : h + 1, begin:span] = log_total[:, h * BLOCK : (h + 1) * BLOCK]
        weights = softmax.astype(jnp.bfloat16)
        prob_grad = lax.dot_general(
            values[0:span, :], grad_rows, nt, preferred_element_type=jnp.float32
        )
        delta = jnp.sum(weights.astype(jnp.float32) * prob_grad, axis=0, keepdims=True)
        score_grad = (softmax * (prob_grad - delta)).astype(jnp.bfloat16)
        output = lax.dot_general(
            value_cols[:, 0:span], weights, nn, preferred_element_type=jnp.float32
        )
        query_sum = lax.dot_general(
            key_cols[:, 0:span], score_grad, nn, preferred_element_type=jnp.float32
        )
        output = jnp.transpose(output.astype(jnp.bfloat16))
        query_sum = jnp.transpose((query_sum * scale).astype(jnp.bfloat16))
        for h in range(heads):
            at = slice(h * BLOCK, (h + 1) * BLOCK)
            attn_out[begin:span, h * head_size : (h + 1) * head_size] = output[at]
            query_grad[begin:span, h * head_size : (h + 1) * head_size] = query_sum[at]
        value_part = lax.dot_general(weights, grad_rows, nn, preferred_element_type=jnp.float32)
        key_part = lax.dot_general(score_grad, query_rows, nn, preferred_element_type=jnp.float32)
        if block == blocks - 1:
            value_sum[...] = value_part
            key_sum[...] = key_part
        else:
            value_sum[0:span, :] += value_part
            key_sum[0:span, :] += key_part
    partial[0] = (key_sum[...] * scale).astype(partial.dtype)
    partial[1] = value_sum[...].astype(partial.dtype)


def attend(order, lengths, queries, keys, values, out_grad):
    slots = lengths.shape[0]
    rows = keys.shape[0] // slots
    head_size = keys.shape[1]
    width = queries.shape[1]
    heads = width // head_size
    wide_spec = pl.BlockSpec((rows, width), lambda i, order, lengths: (order[i], 0))
    narrow_spec = pl.BlockSpec((rows, head_size), lambda i, order, lengths: (order[i], 0))
    return pl.pallas_call(
        functools.partial(slot_body, heads=heads, scale=head_size**-0.5),
        grid_spec=pltpu.PrefetchScalarGridSpec(
            num_scalar_prefetch=2,
            grid=(slots,),
            in_specs=[wide_spec, narrow_spec, narrow_spec, wide_spec],
            out_specs=[
                wide_spec,
                wide_spec,
                pl.BlockSpec((2, rows, head_size), lambda i, order, lengths: (0, order[i], 0)),
                pl.BlockSpec((1, heads, rows), lambda i, order, lengths: (i, 0, 0)),
            ],
            scratch_shapes=[
                pltpu.VMEM((rows, head_size), jnp.float32),
                pltpu.VMEM((rows, head_size), jnp.float32),
            ],
        ),
        out_shape=[
            jax.ShapeDtypeStruct(queries.shape, jnp.bfloat16),
            jax.ShapeDtypeStruct(queries.shape, jnp.bfloat16),
            jax.ShapeDtypeStruct((2,) + keys.shape, jnp.bfloat16),
            jax.ShapeDtypeStruct((slots, heads, rows), jnp.float32),
        ],
        name="attend",
    )(order, lengths, queries, keys, values, out_grad)


def passed_along(block, axis, distance):
    devices = range(lax.axis_size(axis))
    route = [((i - distance) % len(devices), i) for i in devices]
    return lax.ppermute(block, axis, route)


def local(queries, keys, values, out_grad, lengths, hop_table):
    hops = lengths.shape[0]
    cp_count = lax.axis_size("cp")
    dp_count = lax.axis_size("dp")
    hop = jnp.arange(hops, dtype=jnp.int32)
    order = jnp.sum(jnp.where(hop_table[0][None, :] == hop[:, None], hop[None, :], 0), axis=1)
    attn_out, query_grad, partial, stats = attend(
        order.astype(jnp.int32), lengths, queries, keys, values, out_grad
    )
    gathered = [stats[0]] + [
        passed_along(stats[b], "cp", cp_count >> (hops - b)) for b in range(1, hops)
    ]
    row_stats = jnp.concatenate(gathered, axis=1)
    pieces = partial.reshape(dp_count, -1, partial.shape[-1])
    pieces = lax.all_to_all(pieces, "dp", 0, 0)
    first, second, third, fourth = (pieces[i].astype(jnp.float32) for i in range(dp_count))
    piece = ((first + second) + (third + fourth)).astype(jnp.bfloat16)
    whole = lax.all_gather(piece, "dp", axis=0, tiled=True).reshape(partial.shape)
    return (attn_out, query_grad, whole[0], whole[1], row_stats)


def solution(mesh):
    return jax.shard_map(
        local,
        mesh=mesh,
        in_specs=(
            P("cp", "dp"),
            P("cp", None),
            P("cp", None),
            P("cp", "dp"),
            P("cp", None),
            P("cp", None),
        ),
        out_specs=(P("cp", "dp"), P("cp", "dp"), P("cp", None), P("cp", None), P("dp", "cp")),
        check_vma=False,
    )
```

```python
import functools
import math

import jax
import jax.numpy as jnp
from jax import lax
from jax.experimental import pallas as pl
from jax.experimental.pallas import tpu as pltpu
from jax.sharding import PartitionSpec as P


BLOCK = 128
NT = (((1,), (1,)), ((), ()))
NN = (((1,), (0,)), ((), ()))


def matmul(a, b, dims):
    return lax.dot_general(a, b, dims, preferred_element_type=jnp.float32)


def slot_of(hop, hop_table):
    slot = 0
    for s in range(1, hop_table.shape[1]):
        slot = slot + jnp.where(hop_table[0, s] == hop, s, 0)
    return slot


def row_at(block):
    return block * (block + 1) // 2 * BLOCK


def stacked(ref, block, heads, head_size):
    rows = slice(block * BLOCK, (block + 1) * BLOCK)
    return jnp.concatenate(
        [ref[rows, h * head_size : (h + 1) * head_size] for h in range(heads)], axis=0
    )


def key_side(
    hop_table,
    lengths,
    queries,
    keys,
    values,
    out_grad,
    partial,
    weights_out,
    score_grad_out,
    *rest,
    heads,
    scale,
):
    stats = rest[:-2]
    key_sum, value_sum = rest[-2:]
    rows, head_size = keys.shape
    blocks = rows // BLOCK
    wide = heads * BLOCK
    hop = pl.program_id(0)
    slot = slot_of(hop, hop_table)
    first_end = lengths[slot, 0]
    second_end = first_end + lengths[slot, 1]
    third_end = second_end + lengths[slot, 2]
    to_exp2 = scale * math.log2(math.e)
    lane = lax.broadcasted_iota(jnp.int32, (1, wide), 1) % BLOCK
    sublane = lax.broadcasted_iota(jnp.int32, (BLOCK, wide), 0)

    def products(block):
        span = (block + 1) * BLOCK
        query_rows = stacked(queries, block, heads, head_size)
        grad_rows = stacked(out_grad, block, heads, head_size)
        scores = matmul(keys[0:span, :], query_rows, NT)
        prob_grad = matmul(values[0:span, :], grad_rows, NT)
        return scores, prob_grad

    def soften(block, scores, prob_grad):
        begin = block * BLOCK
        row = lane + begin
        start = jnp.where(
            row >= third_end,
            third_end,
            jnp.where(row >= second_end, second_end, jnp.where(row >= first_end, first_end, 0)),
        )
        chunks = []
        peak = None
        for c in range(block + 1):
            allowed = sublane >= start - c * BLOCK
            if c == block:
                allowed = allowed & (sublane <= lane)
            chunk = jnp.where(allowed, scores[c * BLOCK : (c + 1) * BLOCK], -jnp.inf)
            chunks.append(chunk)
            peak = chunk if peak is None else jnp.maximum(peak, chunk)
        row_max = jnp.max(peak, axis=0, keepdims=True)
        total = None
        for c in range(block + 1):
            chunks[c] = jnp.exp2((chunks[c] - row_max) * to_exp2)
            total = chunks[c] if total is None else total + chunks[c]
        row_total = jnp.sum(total, axis=0, keepdims=True)
        share = 1.0 / row_total
        log_total = row_max * scale + jnp.log(row_total)
        for b in range(len(stats)):

            @pl.when(hop == b)
            def _(b=b):
                for h in range(heads):
                    stats[b][h : h + 1, begin : begin + BLOCK] = log_total[
                        :, h * BLOCK : (h + 1) * BLOCK
                    ]

        at = row_at(block)
        total = None
        for c in range(block + 1):
            chunks[c] = chunks[c] * share
            weights = chunks[c].astype(jnp.bfloat16)
            weights_out[0, at + c * BLOCK : at + (c + 1) * BLOCK, :] = weights
            part = weights.astype(jnp.float32) * prob_grad[c * BLOCK : (c + 1) * BLOCK]
            total = part if total is None else total + part
        delta = jnp.sum(total, axis=0, keepdims=True)
        for c in range(block + 1):
            score_grad = chunks[c] * (prob_grad[c * BLOCK : (c + 1) * BLOCK] - delta)
            score_grad_out[0, at + c * BLOCK : at + (c + 1) * BLOCK, :] = score_grad.astype(
                jnp.bfloat16
            )

    def gather_up(block):
        span = (block + 1) * BLOCK
        at = row_at(block)
        query_rows = stacked(queries, block, heads, head_size)
        grad_rows = stacked(out_grad, block, heads, head_size)
        value_part = matmul(weights_out[0, at : at + span, :], grad_rows, NN)
        key_part = matmul(score_grad_out[0, at : at + span, :], query_rows, NN)
        if block == blocks - 1:
            value_sum[...] = value_part
            key_sum[...] = key_part
        else:
            value_sum[0:span, :] += value_part
            key_sum[0:span, :] += key_part

    ready = products(blocks - 1)
    for block in reversed(range(blocks)):
        coming = products(block - 1) if block else None
        if block < blocks - 1:
            gather_up(block + 1)
        soften(block, *ready)
        ready = coming
    gather_up(0)
    partial[0] = (key_sum[...] * scale).astype(partial.dtype)
    partial[1] = value_sum[...].astype(partial.dtype)


def query_side(keys, values, weights, score_grad, attn_out, query_grad, *, heads, scale):
    rows, head_size = keys.shape
    value_cols = jnp.transpose(values[...])
    key_cols = jnp.transpose(keys[...])
    for block in range(rows // BLOCK):
        begin = block * BLOCK
        span = begin + BLOCK
        at = row_at(block)
        output = matmul(value_cols[:, 0:span], weights[0, at : at + span, :], NN)
        query_sum = matmul(key_cols[:, 0:span], score_grad[0, at : at + span, :], NN)
        output = jnp.transpose(output.astype(jnp.bfloat16))
        query_sum = jnp.transpose((query_sum * scale).astype(jnp.bfloat16))
        for h in range(heads):
            at = slice(h * BLOCK, (h + 1) * BLOCK)
            attn_out[begin:span, h * head_size : (h + 1) * head_size] = output[at]
            query_grad[begin:span, h * head_size : (h + 1) * head_size] = query_sum[at]


def key_side_call(hop_table, lengths, queries, keys, values, out_grad):
    slots = lengths.shape[0]
    rows = keys.shape[0] // slots
    head_size = keys.shape[1]
    width = queries.shape[1]
    heads = width // head_size
    wide = heads * BLOCK
    held = row_at(rows // BLOCK)
    at_slot = lambda i, hop_table, lengths: (slot_of(i, hop_table), 0)
    lifted = lambda i, hop_table, lengths: (slot_of(i, hop_table), 0, 0)
    wide_spec = pl.BlockSpec((rows, width), at_slot)
    narrow_spec = pl.BlockSpec((rows, head_size), at_slot)
    stats_spec = pl.BlockSpec((heads, rows), lambda i, hop_table, lengths: (0, 0))
    return pl.pallas_call(
        functools.partial(key_side, heads=heads, scale=head_size**-0.5),
        grid_spec=pltpu.PrefetchScalarGridSpec(
            num_scalar_prefetch=2,
            grid=(slots,),
            in_specs=[wide_spec, narrow_spec, narrow_spec, wide_spec],
            out_specs=[
                pl.BlockSpec(
                    (2, rows, head_size),
                    lambda i, hop_table, lengths: (0, slot_of(i, hop_table), 0),
                ),
                pl.BlockSpec((1, held, wide), lifted),
                pl.BlockSpec((1, held, wide), lifted),
            ]
            + [stats_spec] * slots,
            scratch_shapes=[
                pltpu.VMEM((rows, head_size), jnp.float32),
                pltpu.VMEM((rows, head_size), jnp.float32),
            ],
        ),
        out_shape=[
            jax.ShapeDtypeStruct((2,) + keys.shape, jnp.bfloat16),
            jax.ShapeDtypeStruct((slots, held, wide), jnp.bfloat16),
            jax.ShapeDtypeStruct((slots, held, wide), jnp.bfloat16),
        ]
        + [jax.ShapeDtypeStruct((heads, rows), jnp.float32)] * slots,
        name="key_side",
    )(hop_table, lengths, queries, keys, values, out_grad)


def query_side_call(keys, values, weights, score_grad, heads):
    slots, held, wide = weights.shape
    head_size = keys.shape[1]
    rows = keys.shape[0] // slots
    width = heads * head_size
    wide_spec = pl.BlockSpec((rows, width), lambda i: (i, 0))
    narrow_spec = pl.BlockSpec((rows, head_size), lambda i: (i, 0))
    held_spec = pl.BlockSpec((1, held, wide), lambda i: (i, 0, 0))
    return pl.pallas_call(
        functools.partial(query_side, heads=heads, scale=head_size**-0.5),
        grid=(slots,),
        in_specs=[narrow_spec, narrow_spec, held_spec, held_spec],
        out_specs=[wide_spec, wide_spec],
        out_shape=[jax.ShapeDtypeStruct((keys.shape[0], width), jnp.bfloat16)] * 2,
        name="query_side",
    )(keys, values, weights, score_grad)


def added(pieces, spread):
    total = pieces[0].astype(jnp.float32)
    for i in range(1, pieces.shape[0]):
        total = total + pieces[i].astype(jnp.float32)
    total = total.astype(spread.dtype)
    for i in range(spread.shape[0]):
        spread[i] = total


def added_call(pieces):
    return pl.pallas_call(
        added,
        in_specs=[pl.BlockSpec(memory_space=pltpu.VMEM)],
        out_specs=pl.BlockSpec(memory_space=pltpu.VMEM),
        out_shape=jax.ShapeDtypeStruct(pieces.shape, pieces.dtype),
        compiler_params=pltpu.CompilerParams(vmem_limit_bytes=16 << 20),
        name="added",
    )(pieces)


def passed_along(block, axis, distance):
    devices = range(lax.axis_size(axis))
    route = [((i - distance) % len(devices), i) for i in devices]
    return lax.ppermute(block, axis, route)


def local(queries, keys, values, out_grad, lengths, hop_table):
    heads = queries.shape[1] // keys.shape[1]
    cp_count = lax.axis_size("cp")
    dp_count = lax.axis_size("dp")
    partial, weights, score_grad, *stats = key_side_call(
        hop_table, lengths, queries, keys, values, out_grad
    )
    pieces = partial.reshape(dp_count, -1, partial.shape[-1])
    pieces = lax.all_to_all(pieces, "dp", 0, 0)
    near = passed_along(stats[1], "cp", cp_count >> 2)
    far = passed_along(stats[2], "cp", cp_count >> 1)
    spread = added_call(pieces)
    whole = lax.all_to_all(spread, "dp", 0, 0).reshape(partial.shape)
    attn_out, query_grad = query_side_call(keys, values, weights, score_grad, heads)
    row_stats = jnp.concatenate([stats[0], near, far], axis=1)
    return (attn_out, query_grad, whole[0], whole[1], row_stats)


def solution(mesh):
    return jax.shard_map(
        local,
        mesh=mesh,
        in_specs=(
            P("cp", "dp"),
            P("cp", None),
            P("cp", None),
            P("cp", "dp"),
            P("cp", None),
            P("cp", None),
        ),
        out_specs=(P("cp", "dp"), P("cp", "dp"), P("cp", None), P("cp", None), P("dp", "cp")),
        check_vma=False,
    )
```

```python
import functools
import math

import jax
import jax.numpy as jnp
from jax import lax
from jax.experimental import pallas as pl
from jax.experimental.pallas import tpu as pltpu
from jax.sharding import PartitionSpec as P


BLOCK = 128
NT = (((1,), (1,)), ((), ()))
NN = (((1,), (0,)), ((), ()))


def matmul(a, b, dims):
    return lax.dot_general(a, b, dims, preferred_element_type=jnp.float32)


def slot_of(hop, hop_table):
    slot = 0
    for s in range(1, hop_table.shape[1]):
        slot = slot + jnp.where(hop_table[0, s] == hop, s, 0)
    return slot


def row_at(block):
    return block * (block + 1) // 2 * BLOCK


def stacked(ref, block, heads, head_size):
    rows = slice(block * BLOCK, (block + 1) * BLOCK)
    return jnp.concatenate(
        [ref[rows, h * head_size : (h + 1) * head_size] for h in range(heads)], axis=0
    )


def key_side(
    hop_table,
    lengths,
    queries,
    keys,
    values,
    out_grad,
    partial,
    weights_out,
    score_grad_out,
    *rest,
    heads,
    scale,
):
    kept_stats, moved_stats, key_sum, value_sum, stats = rest
    rows, head_size = keys.shape
    blocks = rows // BLOCK
    wide = heads * BLOCK
    hop = pl.program_id(0)
    slot = slot_of(hop, hop_table)
    first_end = lengths[slot, 0]
    second_end = first_end + lengths[slot, 1]
    third_end = second_end + lengths[slot, 2]
    to_exp2 = scale * math.log2(math.e)
    lane = lax.broadcasted_iota(jnp.int32, (1, wide), 1) % BLOCK
    sublane = lax.broadcasted_iota(jnp.int32, (BLOCK, wide), 0)

    def products(block):
        span = (block + 1) * BLOCK
        query_rows = stacked(queries, block, heads, head_size)
        grad_rows = stacked(out_grad, block, heads, head_size)
        scores = matmul(keys[0:span, :], query_rows, NT)
        prob_grad = matmul(values[0:span, :], grad_rows, NT)
        return scores, prob_grad

    def soften(block, scores, prob_grad):
        begin = block * BLOCK
        row = lane + begin
        start = jnp.where(
            row >= third_end,
            third_end,
            jnp.where(row >= second_end, second_end, jnp.where(row >= first_end, first_end, 0)),
        )
        chunks = []
        peak = None
        for c in range(block + 1):
            allowed = sublane >= start - c * BLOCK
            if c == block:
                allowed = allowed & (sublane <= lane)
            chunk = jnp.where(allowed, scores[c * BLOCK : (c + 1) * BLOCK], -jnp.inf)
            chunks.append(chunk)
            peak = chunk if peak is None else jnp.maximum(peak, chunk)
        row_max = jnp.max(peak, axis=0, keepdims=True)
        total = None
        for c in range(block + 1):
            chunks[c] = jnp.exp2((chunks[c] - row_max) * to_exp2)
            total = chunks[c] if total is None else total + chunks[c]
        row_total = jnp.sum(total, axis=0, keepdims=True)
        share = 1.0 / row_total
        log_total = row_max * scale + jnp.log(row_total)
        for h in range(heads):
            stats[pl.ds(hop, 1), h : h + 1, begin : begin + BLOCK] = log_total[
                None, :, h * BLOCK : (h + 1) * BLOCK
            ]

        at = row_at(block)
        total = None
        for c in range(block + 1):
            chunks[c] = chunks[c] * share
            weights = chunks[c].astype(jnp.bfloat16)
            weights_out[0, at + c * BLOCK : at + (c + 1) * BLOCK, :] = weights
            part = weights.astype(jnp.float32) * prob_grad[c * BLOCK : (c + 1) * BLOCK]
            total = part if total is None else total + part
        delta = jnp.sum(total, axis=0, keepdims=True)
        for c in range(block + 1):
            score_grad = chunks[c] * (prob_grad[c * BLOCK : (c + 1) * BLOCK] - delta)
            score_grad_out[0, at + c * BLOCK : at + (c + 1) * BLOCK, :] = score_grad.astype(
                jnp.bfloat16
            )

    def gather_up(block):
        span = (block + 1) * BLOCK
        at = row_at(block)
        query_rows = stacked(queries, block, heads, head_size)
        grad_rows = stacked(out_grad, block, heads, head_size)
        value_part = matmul(weights_out[0, at : at + span, :], grad_rows, NN)
        key_part = matmul(score_grad_out[0, at : at + span, :], query_rows, NN)
        if block == blocks - 1:
            value_sum[...] = value_part
            key_sum[...] = key_part
        else:
            value_sum[0:span, :] += value_part
            key_sum[0:span, :] += key_part

    ready = products(blocks - 1)
    for block in reversed(range(blocks)):
        coming = products(block - 1) if block else None
        if block < blocks - 1:
            gather_up(block + 1)
        soften(block, *ready)
        ready = coming
    gather_up(0)
    partial[0] = (key_sum[...] * scale).astype(partial.dtype)
    partial[1] = value_sum[...].astype(partial.dtype)

    @pl.when(hop == pl.num_programs(0) - 1)
    def _():
        kept_stats[...] = stats[0]
        moved_stats[...] = stats[1:]


def query_side(keys, values, weights, score_grad, attn_out, query_grad, *, heads, scale):
    rows, head_size = keys.shape
    value_cols = jnp.transpose(values[...])
    key_cols = jnp.transpose(keys[...])
    for block in range(rows // BLOCK):
        begin = block * BLOCK
        span = begin + BLOCK
        at = row_at(block)
        output = matmul(value_cols[:, 0:span], weights[0, at : at + span, :], NN)
        query_sum = matmul(key_cols[:, 0:span], score_grad[0, at : at + span, :], NN)
        output = jnp.transpose(output.astype(jnp.bfloat16))
        query_sum = jnp.transpose((query_sum * scale).astype(jnp.bfloat16))
        for h in range(heads):
            at = slice(h * BLOCK, (h + 1) * BLOCK)
            attn_out[begin:span, h * head_size : (h + 1) * head_size] = output[at]
            query_grad[begin:span, h * head_size : (h + 1) * head_size] = query_sum[at]


def key_side_call(hop_table, lengths, queries, keys, values, out_grad):
    slots = lengths.shape[0]
    rows = keys.shape[0] // slots
    head_size = keys.shape[1]
    width = queries.shape[1]
    heads = width // head_size
    wide = heads * BLOCK
    held = row_at(rows // BLOCK)
    at_slot = lambda i, hop_table, lengths: (slot_of(i, hop_table), 0)
    lifted = lambda i, hop_table, lengths: (slot_of(i, hop_table), 0, 0)
    wide_spec = pl.BlockSpec((rows, width), at_slot)
    narrow_spec = pl.BlockSpec((rows, head_size), at_slot)
    return pl.pallas_call(
        functools.partial(key_side, heads=heads, scale=head_size**-0.5),
        grid_spec=pltpu.PrefetchScalarGridSpec(
            num_scalar_prefetch=2,
            grid=(slots,),
            in_specs=[wide_spec, narrow_spec, narrow_spec, wide_spec],
            out_specs=[
                pl.BlockSpec(
                    (2, rows, head_size),
                    lambda i, hop_table, lengths: (0, slot_of(i, hop_table), 0),
                ),
                pl.BlockSpec((1, held, wide), lifted),
                pl.BlockSpec((1, held, wide), lifted),
            ]
            + [
                pl.BlockSpec((heads, rows), lambda i, hop_table, lengths: (0, 0)),
                pl.BlockSpec((slots - 1, heads, rows), lambda i, hop_table, lengths: (0, 0, 0)),
            ],
            scratch_shapes=[
                pltpu.VMEM((rows, head_size), jnp.float32),
                pltpu.VMEM((rows, head_size), jnp.float32),
                pltpu.VMEM((slots, heads, rows), jnp.float32),
            ],
        ),
        out_shape=[
            jax.ShapeDtypeStruct((2,) + keys.shape, jnp.bfloat16),
            jax.ShapeDtypeStruct((slots, held, wide), jnp.bfloat16),
            jax.ShapeDtypeStruct((slots, held, wide), jnp.bfloat16),
        ]
        + [
            jax.ShapeDtypeStruct((heads, rows), jnp.float32),
            jax.ShapeDtypeStruct((slots - 1, heads, rows), jnp.float32),
        ],
        name="key_side",
    )(hop_table, lengths, queries, keys, values, out_grad)


def query_side_call(keys, values, weights, score_grad, heads):
    slots, held, wide = weights.shape
    head_size = keys.shape[1]
    rows = keys.shape[0] // slots
    width = heads * head_size
    wide_spec = pl.BlockSpec((rows, width), lambda i: (i, 0))
    narrow_spec = pl.BlockSpec((rows, head_size), lambda i: (i, 0))
    held_spec = pl.BlockSpec((1, held, wide), lambda i: (i, 0, 0))
    return pl.pallas_call(
        functools.partial(query_side, heads=heads, scale=head_size**-0.5),
        grid=(slots,),
        in_specs=[narrow_spec, narrow_spec, held_spec, held_spec],
        out_specs=[wide_spec, wide_spec],
        out_shape=[jax.ShapeDtypeStruct((keys.shape[0], width), jnp.bfloat16)] * 2,
        name="query_side",
    )(keys, values, weights, score_grad)


def added(pieces, spread):
    total = pieces[0].astype(jnp.float32)
    for i in range(1, pieces.shape[0]):
        total = total + pieces[i].astype(jnp.float32)
    total = total.astype(spread.dtype)
    for i in range(spread.shape[0]):
        spread[i] = total


def added_call(pieces):
    return pl.pallas_call(
        added,
        in_specs=[pl.BlockSpec(memory_space=pltpu.VMEM)],
        out_specs=pl.BlockSpec(memory_space=pltpu.VMEM),
        out_shape=jax.ShapeDtypeStruct(pieces.shape, pieces.dtype),
        compiler_params=pltpu.CompilerParams(vmem_limit_bytes=16 << 20),
        name="added",
    )(pieces)


def passed_along(block, axis, distance):
    devices = range(lax.axis_size(axis))
    route = [((i - distance) % len(devices), i) for i in devices]
    return lax.ppermute(block, axis, route)


def local(queries, keys, values, out_grad, lengths, hop_table):
    heads = queries.shape[1] // keys.shape[1]
    cp_count = lax.axis_size("cp")
    dp_count = lax.axis_size("dp")
    partial, weights, score_grad, kept_stats, moved_stats = key_side_call(
        hop_table, lengths, queries, keys, values, out_grad
    )
    pieces = partial.reshape(dp_count, -1, partial.shape[-1])
    pieces = lax.all_to_all(pieces, "dp", 0, 0)
    near = passed_along(moved_stats, "cp", cp_count >> 2)
    far = passed_along(near, "cp", cp_count >> 2)
    spread = added_call(pieces)
    whole = lax.all_to_all(spread, "dp", 0, 0).reshape(partial.shape)
    attn_out, query_grad = query_side_call(keys, values, weights, score_grad, heads)
    row_stats = jnp.concatenate([kept_stats, near[0], far[1]], axis=1)
    return (attn_out, query_grad, whole[0], whole[1], row_stats)


def solution(mesh):
    return jax.shard_map(
        local,
        mesh=mesh,
        in_specs=(
            P("cp", "dp"),
            P("cp", None),
            P("cp", None),
            P("cp", "dp"),
            P("cp", None),
            P("cp", None),
        ),
        out_specs=(P("cp", "dp"), P("cp", "dp"), P("cp", None), P("cp", None), P("dp", "cp")),
        check_vma=False,
    )
```

```python
import functools
import math

import jax
import jax.numpy as jnp
from jax import lax
from jax.experimental import pallas as pl
from jax.experimental.pallas import tpu as pltpu
from jax.sharding import PartitionSpec as P


BLOCK = 128
SPLIT = 2
NT = (((1,), (1,)), ((), ()))
NN = (((1,), (0,)), ((), ()))


def matmul(a, b, dims):
    return lax.dot_general(a, b, dims, preferred_element_type=jnp.float32)


def slot_of(hop, hop_table):
    slot = 0
    for s in range(1, hop_table.shape[1]):
        slot = slot + jnp.where(hop_table[0, s] == hop, s, 0)
    return slot


def row_at(block):
    return block * (block + 1) // 2 * BLOCK


def stacked(ref, block, heads, head_size):
    rows = slice(block * BLOCK, (block + 1) * BLOCK)
    return jnp.concatenate(
        [ref[rows, h * head_size : (h + 1) * head_size] for h in range(heads)], axis=0
    )


def key_side(
    hop_table,
    lengths,
    queries,
    keys,
    values,
    out_grad,
    partial,
    weights_out,
    score_grad_out,
    *rest,
    heads,
    scale,
):
    kept_stats, moved_stats, key_sum, value_sum, stats = rest
    rows, head_size = keys.shape
    blocks = rows // BLOCK
    wide = heads * BLOCK
    hop = pl.program_id(0)
    slot = slot_of(hop, hop_table)
    first_end = lengths[slot, 0]
    second_end = first_end + lengths[slot, 1]
    third_end = second_end + lengths[slot, 2]
    to_exp2 = scale * math.log2(math.e)
    lane = lax.broadcasted_iota(jnp.int32, (1, wide), 1) % BLOCK
    sublane = lax.broadcasted_iota(jnp.int32, (BLOCK, wide), 0)

    def products(block):
        span = (block + 1) * BLOCK
        query_rows = stacked(queries, block, heads, head_size)
        grad_rows = stacked(out_grad, block, heads, head_size)
        scores = matmul(keys[0:span, :], query_rows, NT)
        prob_grad = matmul(values[0:span, :], grad_rows, NT)
        return scores, prob_grad

    def soften(block, scores, prob_grad):
        begin = block * BLOCK
        row = lane + begin
        start = jnp.where(
            row >= third_end,
            third_end,
            jnp.where(row >= second_end, second_end, jnp.where(row >= first_end, first_end, 0)),
        )
        chunks = []
        peak = None
        for c in range(block + 1):
            allowed = sublane >= start - c * BLOCK
            if c == block:
                allowed = allowed & (sublane <= lane)
            chunk = jnp.where(allowed, scores[c * BLOCK : (c + 1) * BLOCK], -jnp.inf)
            chunks.append(chunk)
            peak = chunk if peak is None else jnp.maximum(peak, chunk)
        row_max = jnp.max(peak, axis=0, keepdims=True)
        total = None
        for c in range(block + 1):
            chunks[c] = jnp.exp2((chunks[c] - row_max) * to_exp2)
            total = chunks[c] if total is None else total + chunks[c]
        row_total = jnp.sum(total, axis=0, keepdims=True)
        share = 1.0 / row_total
        log_total = row_max * scale + jnp.log(row_total)
        for h in range(heads):
            stats[pl.ds(hop, 1), h : h + 1, begin : begin + BLOCK] = log_total[
                None, :, h * BLOCK : (h + 1) * BLOCK
            ]

        at = row_at(block)
        total = None
        for c in range(block + 1):
            chunks[c] = chunks[c] * share
            weights = chunks[c].astype(jnp.bfloat16)
            weights_out[0, at + c * BLOCK : at + (c + 1) * BLOCK, :] = weights
            part = weights.astype(jnp.float32) * prob_grad[c * BLOCK : (c + 1) * BLOCK]
            total = part if total is None else total + part
        delta = jnp.sum(total, axis=0, keepdims=True)
        for c in range(block + 1):
            score_grad = chunks[c] * (prob_grad[c * BLOCK : (c + 1) * BLOCK] - delta)
            score_grad_out[0, at + c * BLOCK : at + (c + 1) * BLOCK, :] = score_grad.astype(
                jnp.bfloat16
            )

    def gather_up(block):
        span = (block + 1) * BLOCK
        at = row_at(block)
        query_rows = stacked(queries, block, heads, head_size)
        grad_rows = stacked(out_grad, block, heads, head_size)
        value_part = matmul(weights_out[0, at : at + span, :], grad_rows, NN)
        key_part = matmul(score_grad_out[0, at : at + span, :], query_rows, NN)
        if block == blocks - 1:
            value_sum[...] = value_part
            key_sum[...] = key_part
        else:
            value_sum[0:span, :] += value_part
            key_sum[0:span, :] += key_part

    ready = products(blocks - 1)
    for block in reversed(range(blocks)):
        coming = products(block - 1) if block else None
        if block < blocks - 1:
            gather_up(block + 1)
        soften(block, *ready)
        ready = coming
    gather_up(0)
    partial[0] = (key_sum[...] * scale).astype(partial.dtype)
    partial[1] = value_sum[...].astype(partial.dtype)

    @pl.when(hop == pl.num_programs(0) - 1)
    def _():
        kept_stats[...] = stats[0]
        moved_stats[...] = stats[1:]


def query_side(keys, values, weights, score_grad, *rest, heads, scale):
    attn_out, query_grad = rest[-2:]
    rows, head_size = keys.shape
    value_cols = jnp.transpose(values[...])
    key_cols = jnp.transpose(keys[...])
    for block in range(rows // BLOCK):
        begin = block * BLOCK
        span = begin + BLOCK
        at = row_at(block)
        output = matmul(value_cols[:, 0:span], weights[0, at : at + span, :], NN)
        query_sum = matmul(key_cols[:, 0:span], score_grad[0, at : at + span, :], NN)
        output = jnp.transpose(output.astype(jnp.bfloat16))
        query_sum = jnp.transpose((query_sum * scale).astype(jnp.bfloat16))
        for h in range(heads):
            at = slice(h * BLOCK, (h + 1) * BLOCK)
            attn_out[begin:span, h * head_size : (h + 1) * head_size] = output[at]
            query_grad[begin:span, h * head_size : (h + 1) * head_size] = query_sum[at]


def key_side_call(hop_table, lengths, queries, keys, values, out_grad):
    slots = lengths.shape[0]
    rows = keys.shape[0] // slots
    head_size = keys.shape[1]
    width = queries.shape[1]
    heads = width // head_size
    wide = heads * BLOCK
    held = row_at(rows // BLOCK)
    at_slot = lambda i, hop_table, lengths: (slot_of(i, hop_table), 0)
    lifted = lambda i, hop_table, lengths: (slot_of(i, hop_table), 0, 0)
    wide_spec = pl.BlockSpec((rows, width), at_slot)
    narrow_spec = pl.BlockSpec((rows, head_size), at_slot)
    return pl.pallas_call(
        functools.partial(key_side, heads=heads, scale=head_size**-0.5),
        grid_spec=pltpu.PrefetchScalarGridSpec(
            num_scalar_prefetch=2,
            grid=(slots,),
            in_specs=[wide_spec, narrow_spec, narrow_spec, wide_spec],
            out_specs=[
                pl.BlockSpec(
                    (2, rows, head_size),
                    lambda i, hop_table, lengths: (0, slot_of(i, hop_table), 0),
                ),
                pl.BlockSpec((1, held, wide), lifted),
                pl.BlockSpec((1, held, wide), lifted),
            ]
            + [
                pl.BlockSpec((heads, rows), lambda i, hop_table, lengths: (0, 0)),
                pl.BlockSpec((slots - 1, heads, rows), lambda i, hop_table, lengths: (0, 0, 0)),
            ],
            scratch_shapes=[
                pltpu.VMEM((rows, head_size), jnp.float32),
                pltpu.VMEM((rows, head_size), jnp.float32),
                pltpu.VMEM((slots, heads, rows), jnp.float32),
            ],
        ),
        out_shape=[
            jax.ShapeDtypeStruct((2,) + keys.shape, jnp.bfloat16),
            jax.ShapeDtypeStruct((slots, held, wide), jnp.bfloat16),
            jax.ShapeDtypeStruct((slots, held, wide), jnp.bfloat16),
        ]
        + [
            jax.ShapeDtypeStruct((heads, rows), jnp.float32),
            jax.ShapeDtypeStruct((slots - 1, heads, rows), jnp.float32),
        ],
        name="key_side",
    )(hop_table, lengths, queries, keys, values, out_grad)


def query_side_call(keys, values, weights, score_grad, heads, begin, end, earlier=()):
    slots, held, wide = weights.shape
    head_size = keys.shape[1]
    rows = keys.shape[0] // slots
    width = heads * head_size
    wide_spec = pl.BlockSpec((rows, width), lambda i: (begin + i, 0))
    narrow_spec = pl.BlockSpec((rows, head_size), lambda i: (begin + i, 0))
    held_spec = pl.BlockSpec((1, held, wide), lambda i: (begin + i, 0, 0))
    return pl.pallas_call(
        functools.partial(query_side, heads=heads, scale=head_size**-0.5),
        grid=(end - begin,),
        in_specs=[narrow_spec, narrow_spec, held_spec, held_spec]
        + [pl.BlockSpec(memory_space=pl.ANY)] * len(earlier),
        out_specs=[wide_spec, wide_spec],
        out_shape=[jax.ShapeDtypeStruct((keys.shape[0], width), jnp.bfloat16)] * 2,
        input_output_aliases={4: 0, 5: 1} if earlier else {},
        name="query_side",
    )(keys, values, weights, score_grad, *earlier)


def added(pieces, spread, total, sems):
    size = pieces.shape[1] // 2
    copies = []
    for half in range(2):
        rows = slice(half * size, (half + 1) * size)
        own = pieces[0, rows].astype(jnp.float32)
        for i in range(1, pieces.shape[0]):
            own = own + pieces[i, rows].astype(jnp.float32)
        total[rows] = own.astype(total.dtype)
        for i in range(spread.shape[0]):
            copy = pltpu.make_async_copy(
                total.at[pl.ds(half * size, size)],
                spread.at[i, pl.ds(half * size, size)],
                sems.at[half, i],
            )
            copy.start()
            copies.append(copy)
    for copy in copies:
        copy.wait()


def added_call(pieces):
    return pl.pallas_call(
        added,
        in_specs=[pl.BlockSpec(memory_space=pltpu.VMEM)],
        out_specs=pl.BlockSpec(memory_space=pl.ANY),
        out_shape=jax.ShapeDtypeStruct(pieces.shape, pieces.dtype),
        scratch_shapes=[
            pltpu.VMEM(pieces.shape[1:], pieces.dtype),
            pltpu.SemaphoreType.DMA((2, pieces.shape[0])),
        ],
        compiler_params=pltpu.CompilerParams(vmem_limit_bytes=16 << 20),
        name="added",
    )(pieces)


def passed_along(block, axis, distance):
    devices = range(lax.axis_size(axis))
    route = [((i - distance) % len(devices), i) for i in devices]
    return lax.ppermute(block, axis, route)


def finish(whole, kept, near, far, key_grad, value_grad, row_stats, sems):
    half = whole.shape[0] // 2
    rows = kept.shape[1]
    copies = [
        (whole.at[pl.ds(0, half)], key_grad),
        (whole.at[pl.ds(half, half)], value_grad),
        (kept, row_stats.at[:, pl.ds(0, rows)]),
        (near.at[0], row_stats.at[:, pl.ds(rows, rows)]),
        (far.at[1], row_stats.at[:, pl.ds(2 * rows, rows)]),
    ]
    started = [
        pltpu.make_async_copy(source, target, sems.at[i])
        for i, (source, target) in enumerate(copies)
    ]
    for copy in started:
        copy.start()
    for copy in started:
        copy.wait()


def finish_call(whole, kept, near, far):
    parts, size, head_size = whole.shape
    half = jax.ShapeDtypeStruct((parts // 2, size, head_size), whole.dtype)
    return pl.pallas_call(
        finish,
        in_specs=[pl.BlockSpec(memory_space=pltpu.VMEM)] * 4,
        out_specs=[pl.BlockSpec(memory_space=pl.ANY)] * 3,
        out_shape=[
            half,
            half,
            jax.ShapeDtypeStruct((kept.shape[0], 3 * kept.shape[1]), kept.dtype),
        ],
        scratch_shapes=[pltpu.SemaphoreType.DMA((5,))],
        compiler_params=pltpu.CompilerParams(vmem_limit_bytes=16 << 20),
        name="finish",
    )(whole, kept, near, far)


def local(queries, keys, values, out_grad, lengths, hop_table):
    hops = lengths.shape[0]
    heads = queries.shape[1] // keys.shape[1]
    cp_count = lax.axis_size("cp")
    dp_count = lax.axis_size("dp")
    partial, weights, score_grad, kept_stats, moved_stats = key_side_call(
        hop_table, lengths, queries, keys, values, out_grad
    )
    pieces = partial.reshape(dp_count, -1, partial.shape[-1])
    pieces = lax.all_to_all(pieces, "dp", 0, 0)
    near = passed_along(moved_stats, "cp", cp_count >> 2)
    far = passed_along(near, "cp", cp_count >> 2)
    spread = added_call(pieces)
    whole = lax.all_to_all(spread, "dp", 0, 0)
    query_parts = query_side_call(keys, values, weights, score_grad, heads, 0, SPLIT)
    attn_out, query_grad = query_side_call(
        keys, values, weights, score_grad, heads, SPLIT, hops, query_parts
    )
    key_grad, value_grad, row_stats = finish_call(whole, kept_stats, near, far)
    return (
        attn_out,
        query_grad,
        key_grad.reshape(keys.shape),
        value_grad.reshape(values.shape),
        row_stats,
    )


def solution(mesh):
    return jax.shard_map(
        local,
        mesh=mesh,
        in_specs=(
            P("cp", "dp"),
            P("cp", None),
            P("cp", None),
            P("cp", "dp"),
            P("cp", None),
            P("cp", None),
        ),
        out_specs=(P("cp", "dp"), P("cp", "dp"), P("cp", None), P("cp", None), P("dp", "cp")),
        check_vma=False,
    )
```

```python
import functools
import math

import jax
import jax.numpy as jnp
from jax import lax
from jax.experimental import pallas as pl
from jax.experimental.pallas import tpu as pltpu
from jax.sharding import PartitionSpec as P


BLOCK = 128
SPLIT = 1
NT = (((1,), (1,)), ((), ()))
NN = (((1,), (0,)), ((), ()))


def matmul(a, b, dims):
    return lax.dot_general(a, b, dims, preferred_element_type=jnp.float32)


def slot_of(hop, hop_table):
    slot = 0
    for s in range(1, hop_table.shape[1]):
        slot = slot + jnp.where(hop_table[0, s] == hop, s, 0)
    return slot


def row_at(block):
    return block * (block + 1) // 2 * BLOCK


def stacked(ref, block, heads, head_size):
    rows = slice(block * BLOCK, (block + 1) * BLOCK)
    return jnp.concatenate(
        [ref[rows, h * head_size : (h + 1) * head_size] for h in range(heads)], axis=0
    )


def key_side(
    hop_table,
    lengths,
    queries,
    keys,
    values,
    out_grad,
    partial,
    weights_out,
    score_grad_out,
    *rest,
    heads,
    scale,
):
    kept_stats, moved_stats, key_sum, value_sum, stats = rest
    rows, head_size = keys.shape
    blocks = rows // BLOCK
    wide = heads * BLOCK
    hop = pl.program_id(0)
    slot = slot_of(hop, hop_table)
    first_end = lengths[slot, 0]
    second_end = first_end + lengths[slot, 1]
    third_end = second_end + lengths[slot, 2]
    to_exp2 = scale * math.log2(math.e)
    lane = lax.broadcasted_iota(jnp.int32, (1, wide), 1) % BLOCK
    sublane = lax.broadcasted_iota(jnp.int32, (BLOCK, wide), 0)

    def products(block):
        span = (block + 1) * BLOCK
        query_rows = stacked(queries, block, heads, head_size)
        grad_rows = stacked(out_grad, block, heads, head_size)
        scores = matmul(keys[0:span, :], query_rows, NT)
        prob_grad = matmul(values[0:span, :], grad_rows, NT)
        return scores, prob_grad

    def soften(block, scores, prob_grad):
        begin = block * BLOCK
        row = lane + begin
        start = jnp.where(
            row >= third_end,
            third_end,
            jnp.where(row >= second_end, second_end, jnp.where(row >= first_end, first_end, 0)),
        )
        chunks = []
        peak = None
        for c in range(block + 1):
            allowed = sublane >= start - c * BLOCK
            if c == block:
                allowed = allowed & (sublane <= lane)
            chunk = jnp.where(allowed, scores[c * BLOCK : (c + 1) * BLOCK], -jnp.inf)
            chunks.append(chunk)
            peak = chunk if peak is None else jnp.maximum(peak, chunk)
        row_max = jnp.max(peak, axis=0, keepdims=True)
        total = None
        for c in range(block + 1):
            chunks[c] = jnp.exp2((chunks[c] - row_max) * to_exp2)
            total = chunks[c] if total is None else total + chunks[c]
        row_total = jnp.sum(total, axis=0, keepdims=True)
        share = 1.0 / row_total
        log_total = row_max * scale + jnp.log(row_total)
        for h in range(heads):
            stats[pl.ds(hop, 1), h : h + 1, begin : begin + BLOCK] = log_total[
                None, :, h * BLOCK : (h + 1) * BLOCK
            ]

        at = row_at(block)
        total = None
        for c in range(block + 1):
            chunks[c] = chunks[c] * share
            weights = chunks[c].astype(jnp.bfloat16)
            weights_out[0, at + c * BLOCK : at + (c + 1) * BLOCK, :] = weights
            part = weights.astype(jnp.float32) * prob_grad[c * BLOCK : (c + 1) * BLOCK]
            total = part if total is None else total + part
        delta = jnp.sum(total, axis=0, keepdims=True)
        for c in range(block + 1):
            score_grad = chunks[c] * (prob_grad[c * BLOCK : (c + 1) * BLOCK] - delta)
            score_grad_out[0, at + c * BLOCK : at + (c + 1) * BLOCK, :] = score_grad.astype(
                jnp.bfloat16
            )

    def gather_up(block):
        span = (block + 1) * BLOCK
        at = row_at(block)
        query_rows = stacked(queries, block, heads, head_size)
        grad_rows = stacked(out_grad, block, heads, head_size)
        value_part = matmul(weights_out[0, at : at + span, :], grad_rows, NN)
        key_part = matmul(score_grad_out[0, at : at + span, :], query_rows, NN)
        if block == blocks - 1:
            value_sum[...] = value_part
            key_sum[...] = key_part
        else:
            value_sum[0:span, :] += value_part
            key_sum[0:span, :] += key_part

    ready = products(blocks - 1)
    for block in reversed(range(blocks)):
        coming = products(block - 1) if block else None
        if block < blocks - 1:
            gather_up(block + 1)
        soften(block, *ready)
        ready = coming
    gather_up(0)
    partial[0] = (key_sum[...] * scale).astype(partial.dtype)
    partial[1] = value_sum[...].astype(partial.dtype)

    @pl.when(hop == pl.num_programs(0) - 1)
    def _():
        kept_stats[...] = stats[0]
        moved_stats[...] = stats[1:]


def query_side(keys, values, weights, score_grad, *rest, heads, scale):
    attn_out, query_grad = rest[-2:]
    rows, head_size = keys.shape
    value_cols = jnp.transpose(values[...])
    key_cols = jnp.transpose(keys[...])
    for block in range(rows // BLOCK):
        begin = block * BLOCK
        span = begin + BLOCK
        at = row_at(block)
        output = matmul(value_cols[:, 0:span], weights[0, at : at + span, :], NN)
        query_sum = matmul(key_cols[:, 0:span], score_grad[0, at : at + span, :], NN)
        output = jnp.transpose(output.astype(jnp.bfloat16))
        query_sum = jnp.transpose((query_sum * scale).astype(jnp.bfloat16))
        for h in range(heads):
            at = slice(h * BLOCK, (h + 1) * BLOCK)
            attn_out[begin:span, h * head_size : (h + 1) * head_size] = output[at]
            query_grad[begin:span, h * head_size : (h + 1) * head_size] = query_sum[at]


def key_side_call(hop_table, lengths, queries, keys, values, out_grad):
    slots = lengths.shape[0]
    rows = keys.shape[0] // slots
    head_size = keys.shape[1]
    width = queries.shape[1]
    heads = width // head_size
    wide = heads * BLOCK
    held = row_at(rows // BLOCK)
    at_slot = lambda i, hop_table, lengths: (slot_of(i, hop_table), 0)
    lifted = lambda i, hop_table, lengths: (slot_of(i, hop_table), 0, 0)
    wide_spec = pl.BlockSpec((rows, width), at_slot)
    narrow_spec = pl.BlockSpec((rows, head_size), at_slot)
    return pl.pallas_call(
        functools.partial(key_side, heads=heads, scale=head_size**-0.5),
        grid_spec=pltpu.PrefetchScalarGridSpec(
            num_scalar_prefetch=2,
            grid=(slots,),
            in_specs=[wide_spec, narrow_spec, narrow_spec, wide_spec],
            out_specs=[
                pl.BlockSpec(
                    (2, rows, head_size),
                    lambda i, hop_table, lengths: (0, slot_of(i, hop_table), 0),
                ),
                pl.BlockSpec((1, held, wide), lifted),
                pl.BlockSpec((1, held, wide), lifted),
            ]
            + [
                pl.BlockSpec((heads, rows), lambda i, hop_table, lengths: (0, 0)),
                pl.BlockSpec((slots - 1, heads, rows), lambda i, hop_table, lengths: (0, 0, 0)),
            ],
            scratch_shapes=[
                pltpu.VMEM((rows, head_size), jnp.float32),
                pltpu.VMEM((rows, head_size), jnp.float32),
                pltpu.VMEM((slots, heads, rows), jnp.float32),
            ],
        ),
        out_shape=[
            jax.ShapeDtypeStruct((2,) + keys.shape, jnp.bfloat16),
            jax.ShapeDtypeStruct((slots, held, wide), jnp.bfloat16),
            jax.ShapeDtypeStruct((slots, held, wide), jnp.bfloat16),
        ]
        + [
            jax.ShapeDtypeStruct((heads, rows), jnp.float32),
            jax.ShapeDtypeStruct((slots - 1, heads, rows), jnp.float32),
        ],
        name="key_side",
    )(hop_table, lengths, queries, keys, values, out_grad)


def query_side_call(keys, values, weights, score_grad, heads, begin, end, earlier=()):
    slots, held, wide = weights.shape
    head_size = keys.shape[1]
    rows = keys.shape[0] // slots
    width = heads * head_size
    wide_spec = pl.BlockSpec((rows, width), lambda i: (begin + i, 0))
    narrow_spec = pl.BlockSpec((rows, head_size), lambda i: (begin + i, 0))
    held_spec = pl.BlockSpec((1, held, wide), lambda i: (begin + i, 0, 0))
    return pl.pallas_call(
        functools.partial(query_side, heads=heads, scale=head_size**-0.5),
        grid=(end - begin,),
        in_specs=[narrow_spec, narrow_spec, held_spec, held_spec]
        + [pl.BlockSpec(memory_space=pl.ANY)] * len(earlier),
        out_specs=[wide_spec, wide_spec],
        out_shape=[jax.ShapeDtypeStruct((keys.shape[0], width), jnp.bfloat16)] * 2,
        input_output_aliases={4: 0, 5: 1} if earlier else {},
        name="query_side",
    )(keys, values, weights, score_grad, *earlier)


def added(pieces, spread):
    total = pieces[0].astype(jnp.float32)
    for i in range(1, pieces.shape[0]):
        total = total + pieces[i].astype(jnp.float32)
    total = total.astype(spread.dtype)
    for i in range(spread.shape[0]):
        spread[i] = total


def added_call(pieces):
    return pl.pallas_call(
        added,
        in_specs=[pl.BlockSpec(memory_space=pltpu.VMEM)],
        out_specs=pl.BlockSpec(memory_space=pltpu.VMEM),
        out_shape=jax.ShapeDtypeStruct(pieces.shape, pieces.dtype),
        compiler_params=pltpu.CompilerParams(vmem_limit_bytes=16 << 20),
        name="added",
    )(pieces)


def passed_along(block, axis, distance):
    devices = range(lax.axis_size(axis))
    route = [((i - distance) % len(devices), i) for i in devices]
    return lax.ppermute(block, axis, route)


def finish(whole, kept, near, far, key_grad, value_grad, row_stats, sems):
    half = whole.shape[0] // 2
    rows = kept.shape[1]
    copies = [
        (whole.at[pl.ds(0, half)], key_grad),
        (whole.at[pl.ds(half, half)], value_grad),
        (kept, row_stats.at[:, pl.ds(0, rows)]),
        (near.at[0], row_stats.at[:, pl.ds(rows, rows)]),
        (far.at[1], row_stats.at[:, pl.ds(2 * rows, rows)]),
    ]
    started = [
        pltpu.make_async_copy(source, target, sems.at[i])
        for i, (source, target) in enumerate(copies)
    ]
    for copy in started:
        copy.start()
    for copy in started:
        copy.wait()


def finish_call(whole, kept, near, far):
    parts, size, head_size = whole.shape
    half = jax.ShapeDtypeStruct((parts // 2, size, head_size), whole.dtype)
    return pl.pallas_call(
        finish,
        in_specs=[pl.BlockSpec(memory_space=pltpu.VMEM)] * 4,
        out_specs=[pl.BlockSpec(memory_space=pl.ANY)] * 3,
        out_shape=[
            half,
            half,
            jax.ShapeDtypeStruct((kept.shape[0], 3 * kept.shape[1]), kept.dtype),
        ],
        scratch_shapes=[pltpu.SemaphoreType.DMA((5,))],
        compiler_params=pltpu.CompilerParams(vmem_limit_bytes=16 << 20),
        name="finish",
    )(whole, kept, near, far)


def local(queries, keys, values, out_grad, lengths, hop_table):
    hops = lengths.shape[0]
    heads = queries.shape[1] // keys.shape[1]
    cp_count = lax.axis_size("cp")
    dp_count = lax.axis_size("dp")
    partial, weights, score_grad, kept_stats, moved_stats = key_side_call(
        hop_table, lengths, queries, keys, values, out_grad
    )
    pieces = partial.reshape(dp_count, -1, partial.shape[-1])
    pieces = lax.all_to_all(pieces, "dp", 0, 0)
    near = passed_along(moved_stats, "cp", cp_count >> 2)
    far = passed_along(near, "cp", cp_count >> 2)
    spread = added_call(pieces)
    whole = lax.all_to_all(spread, "dp", 0, 0)
    query_parts = query_side_call(keys, values, weights, score_grad, heads, 0, SPLIT)
    attn_out, query_grad = query_side_call(
        keys, values, weights, score_grad, heads, SPLIT, hops, query_parts
    )
    key_grad, value_grad, row_stats = finish_call(whole, kept_stats, near, far)
    return (
        attn_out,
        query_grad,
        key_grad.reshape(keys.shape),
        value_grad.reshape(values.shape),
        row_stats,
    )


def solution(mesh):
    return jax.shard_map(
        local,
        mesh=mesh,
        in_specs=(
            P("cp", "dp"),
            P("cp", None),
            P("cp", None),
            P("cp", "dp"),
            P("cp", None),
            P("cp", None),
        ),
        out_specs=(P("cp", "dp"), P("cp", "dp"), P("cp", None), P("cp", None), P("dp", "cp")),
        check_vma=False,
    )
```
